32 devices in a mesh: tile: 4 (over y, core), quad: 8 (over z, x).
Axes of the slice: x: 2, y: 2, z: 4, core: 2. Of those that a mesh axis runs over, the one named last changes fastest.
Arguments:
- adjoint_next: float32 [32, 32, 512], P('quad', None, 'tile'), may hold values from -6 to 6
- saved_state: float32 [32, 32, 512], P('quad', None, 'tile'), may hold values from 0.2 to 2
- gain_left: float32 [8, 32, 1024], P('quad'), may hold values from 0.1 to 2
- gain_right: float32 [8, 32, 1024], P('quad'), may hold values from 0.1 to 2
Outputs:
- adjoint_prev: float32 [32, 32, 512], P('quad', None, 'tile')
The draws below stay inside these ranges and needn't reach their ends.
All inputs are finite; a program needn't handle non-finite values.
Results may differ from the reference program's by a relative error of at most 0.0001.
Values sent between devices are 32-bit elements; how exact they have to be, the bound alone decides.
No kernel may reach another device: no remote copies, remote signals or barrier semaphores. Data moves between devices by JAX's collectives and lax.ppermute only.
A program may use at most 64 MiB of HBM per device.

```python
import math
import jax
import jax.numpy as jnp
from jax import lax

NV = 32
CY = 2
PAIRS = 8
NXC = 8


def shard_levels(own_key, shape, split, least, high):
    factor_of, own = 1.0, jax.random.fold_in(own_key, 6)
    for position, parts in split:
        steps = jnp.exp(jax.random.uniform(jax.random.fold_in(own, position), (parts,), jnp.float32, least / len(split), high / len(split)))
        factor_of = factor_of * jnp.repeat(steps, shape[position] // parts).reshape([-1 if axis == position else 1 for axis in range(len(shape))])
    return factor_of


def centred(stream_key, extent, deviation, most, cuts=(), kind=jnp.bfloat16):
    entries = jax.random.normal(stream_key, extent, jnp.float32) * deviation
    if len(cuts) > 0:
        entries = shard_levels(stream_key, extent, cuts, -0.22, 0.18) * entries
    return jnp.clip(entries, min=-most, max=most).astype(kind)


def setup_inputs(seed: int = 0) -> dict:
    key_list = jax.random.split(jax.random.key(seed), 5)
    adjoint_next = centred(key_list[0], (NV, NV, NXC * CY * NV), 1.0, 6.0, ((0, 8), (2, 4)), jnp.float32)
    saved_state = jnp.clip(0.2 + 1.8 * jax.random.uniform(key_list[1], (NV, NV, NXC * CY * NV), jnp.float32) ** shard_levels(key_list[1], (NV, NV, NXC * CY * NV), ((0, 8), (2, 4)), -0.2, 0.2), 0.2, 2.0)
    gain_left = jnp.clip(jnp.exp(math.log(2.0) - 2.9957323 * jax.random.uniform(key_list[2], (PAIRS, NV, NV * NV), jnp.float32) ** shard_levels(key_list[2], (PAIRS, NV, NV * NV), ((0, 8),), -0.2, 0.2)), 0.1, 2.0)
    gain_right = jnp.clip(jnp.exp(math.log(2.0) - 2.9957323 * jax.random.uniform(key_list[3], (PAIRS, NV, NV * NV), jnp.float32) ** shard_levels(key_list[3], (PAIRS, NV, NV * NV), ((0, 8),), -0.2, 0.2)), 0.1, 2.0)
    return dict(adjoint_next=adjoint_next, saved_state=saved_state, gain_left=gain_left, gain_right=gain_right)


def stream_axis(values, along, courant):
    ahead_one = jnp.roll(values, -1, along)
    ahead_two = jnp.roll(values, -2, along)
    behind_one = jnp.roll(values, 1, along)
    behind_two = jnp.roll(values, 2, along)
    upwind = jnp.maximum(courant, 0.0) * (3.0 * values - 4.0 * ahead_one + ahead_two) / 2.0
    downwind = jnp.minimum(courant, 0.0) * (3.0 * values - 4.0 * behind_one + behind_two) / 2.0
    return downwind - upwind


def even_half(multiplier):
    flip_axes = (0, 1, 2)
    mirrored = jnp.roll(jnp.flip(multiplier, flip_axes), 1, flip_axes)
    return ((multiplier + mirrored) * 0.5)[:, :, : NV // 2 + 1]


def reference(adjoint_next, saved_state, gain_left, gain_right):
    adjoint_grid = adjoint_next.reshape(NV, NV, NXC, CY, NV)
    state_grid = saved_state.reshape(NV, NV, NXC, CY, NV)
    speeds = (jnp.arange(NV, dtype=jnp.float32) - (NV - 1) / 2.0) / NV
    courant_x = speeds.reshape(NV, 1, 1, 1, 1)
    courant_y = speeds.reshape(1, NV, 1, 1, 1)
    passed = adjoint_grid + stream_axis(adjoint_grid, 2, courant_x) + stream_axis(adjoint_grid, 3, courant_y)
    cell_count = NXC * CY
    adjoint_cells = jnp.transpose(passed, (2, 3, 0, 1, 4)).reshape(cell_count, NV, NV, NV)
    state_cells = jnp.transpose(state_grid, (2, 3, 0, 1, 4)).reshape(cell_count, NV, NV, NV)
    left_tables = gain_left.reshape(PAIRS, NV, NV, NV)
    right_tables = gain_right.reshape(PAIRS, NV, NV, NV)
    spectral_axes = (1, 2, 3)
    velocity_shape = (NV, NV, NV)
    spectrum = jnp.fft.rfftn(state_cells, axes=spectral_axes)
    product = jnp.fft.rfftn(state_cells * adjoint_cells, axes=spectral_axes)

    def per_pair(totals, pair_items):
        left_full, right_full = pair_items
        left_one = even_half(left_full)
        right_one = even_half(right_full)
        loss_one = even_half(left_full * right_full)
        filtered_left = jnp.fft.irfftn(spectrum * left_one, s=velocity_shape, axes=spectral_axes)
        filtered_right = jnp.fft.irfftn(spectrum * right_one, s=velocity_shape, axes=spectral_axes)
        pair_term = (left_one * jnp.fft.rfftn(adjoint_cells * filtered_right, axes=spectral_axes)
                     + right_one * jnp.fft.rfftn(adjoint_cells * filtered_left, axes=spectral_axes)
                     - loss_one * product)
        return (totals[0] + jnp.real(pair_term), totals[1] + jnp.imag(pair_term)), None

    empty_sum = jnp.zeros(spectrum.shape, jnp.float32)
    (total_real, total_imag), _ = lax.scan(per_pair, (empty_sum, empty_sum), (left_tables, right_tables))
    loss_table = even_half(jnp.sum(left_tables * right_tables, axis=0))
    loss_field = jnp.fft.irfftn(spectrum * loss_table, s=velocity_shape, axes=spectral_axes)
    collision = jnp.fft.irfftn(lax.complex(total_real, total_imag), s=velocity_shape, axes=spectral_axes) - adjoint_cells * loss_field
    result_cells = adjoint_cells + collision / PAIRS
    result_grid = jnp.transpose(result_cells.reshape(NXC, CY, NV, NV, NV), (2, 3, 0, 1, 4))
    return result_grid.reshape(NV, NV, NXC * CY * NV)
```

```python
import functools

import jax
import jax.numpy as jnp
import numpy as np
from jax import lax
from jax.experimental import pallas as pl
from jax.experimental.pallas import tpu as pltpu
from jax.sharding import PartitionSpec as P


F32 = jnp.float32
BF16 = jnp.bfloat16
VMEM = pl.BlockSpec(memory_space=pltpu.VMEM)
SMEM = pl.BlockSpec(memory_space=pltpu.SMEM)


def split_np(table):
    high = np.asarray(table, np.float32).astype(BF16)
    low = (np.asarray(table, np.float64) - high.astype(np.float64)).astype(BF16)
    return high, low


def make_constants(length, n):
    m = length // n
    lanes = n * length
    b2, c = np.divmod(np.arange(lanes), length)
    turns = np.outer(b2, b2) % n / n + np.outer(c, c) % length / length
    er, ei = np.cos(2 * np.pi * turns), -np.sin(2 * np.pi * turns)
    lane_fwd = np.block([[er, ei], [-ei, er]])
    lane_inv = np.block([[er, -ei], [ei, er]])
    a = np.arange(length)
    turns = np.outer(a, a) % length / length
    co, si = np.cos(2 * np.pi * turns), np.sin(2 * np.pi * turns)
    row_fwd = np.block([[co, si], [-si, co]])
    row_inv = np.block([[co, -si], [si, co]]) / float(length**3)

    def lane(table):
        high, low = split_np(table)
        return np.concatenate([high, high, low], axis=0)

    def row(table):
        high, low = split_np(table)
        return np.concatenate([high, high, low], axis=1)

    theta = 2 * np.pi * np.outer(np.arange(m), b2) / length
    twiddle = np.concatenate([np.cos(theta), np.sin(theta)], axis=0).astype(np.float32)
    return dict(
        lane_real=lane(lane_fwd[:lanes]),
        lane_fwd=lane(lane_fwd),
        lane_inv=lane(lane_inv),
        row_fwd=row(row_fwd),
        row_inv=row(row_inv),
        twiddle=twiddle,
    )


def make_mirrors(length, n):
    lanes = n * length
    l, c = np.divmod(np.arange(lanes), length)
    source = np.where(l == 0, 0, lanes) + (-l) % n * length + (-c) % length
    lane_mirror = np.zeros((2 * lanes, lanes), np.float32)
    lane_mirror[source, np.arange(lanes)] = 1.0
    row_mirror = np.zeros((length, length), np.float32)
    row_mirror[np.arange(length), (-np.arange(length)) % length] = 1.0
    return lane_mirror, row_mirror


def swap_groups(vectors, length):
    v0, v1, v2, v3 = vectors
    lane = lax.broadcasted_iota(jnp.int32, v0.shape, v0.ndim - 1)
    low = lane < 2 * length
    even = lane // length % 2 == 0
    roll = functools.partial(pltpu.roll, axis=v0.ndim - 1)
    a0, a2 = jnp.where(low, v0, roll(v2, 2 * length)), jnp.where(low, roll(v0, 2 * length), v2)
    a1, a3 = jnp.where(low, v1, roll(v3, 2 * length)), jnp.where(low, roll(v1, 2 * length), v3)
    b0, b1 = jnp.where(even, a0, roll(a1, length)), jnp.where(even, roll(a0, 3 * length), a1)
    b2, b3 = jnp.where(even, a2, roll(a3, length)), jnp.where(even, roll(a2, 3 * length), a3)
    return b0, b1, b2, b3


def even_kernel(left_ref, right_ref, lane_ref, row_ref, out_ref):
    left, right = left_ref[...], right_ref[...]
    length = left.shape[0]
    lanes = lane_ref.shape[1]
    groups = left.shape[1] // lanes
    for i, table in enumerate((left, right, left * right)):
        tiles = [table[:, g * lanes : (g + 1) * lanes] for g in range(groups)]
        parts = []
        for g in range(groups):
            pair = jnp.concatenate([tiles[-g % groups], tiles[(-g - 1) % groups]], axis=1)
            parts.append(jnp.dot(pair, lane_ref[...], precision=lax.Precision.HIGHEST, preferred_element_type=F32))
        mirrored = jnp.dot(row_ref[...], jnp.concatenate(parts, axis=1), precision=lax.Precision.HIGHEST, preferred_element_type=F32)
        out_ref[i] = 0.5 * (table + mirrored)


def pass_kernel(first_ref, ahead_ref, adjoint_ref, state_ref, halo_ref, passed_ref, packed_ref):
    planes, length, lanes = adjoint_ref.shape
    n = lanes // length
    m = length // n
    copies = packed_ref.shape[0] // n
    lane = lax.broadcasted_iota(jnp.int32, (length, lanes), 1)
    b = lax.broadcasted_iota(jnp.int32, (length, lanes), 0)
    sy = (b.astype(F32) - (length - 1) / 2.0) / length
    ahead = ahead_ref[0]
    own_lanes = jnp.where(ahead == 1, lane, lanes - 1 - lane) < lanes // 2
    odd = lane // length % 2 == 1
    for a in range(planes):
        centre, two = adjoint_ref[a], halo_ref[a]
        one = jnp.where(own_lanes, pltpu.roll(centre, lanes // 2, axis=1), pltpu.roll(two, lanes // 2, axis=1))
        partner = jnp.where(odd, pltpu.roll(centre, length, axis=1), pltpu.roll(centre, lanes - length, axis=1))
        sx = (first_ref[0] + float(a) - (length - 1) / 2.0) / length
        passed = centre - jnp.abs(sx) * (3.0 * centre - 4.0 * one + two) / 2.0 - 2.0 * jnp.abs(sy) * (centre - partner)
        passed_ref[a] = passed
        for f, field in enumerate((state_ref[a], passed)):
            cells = swap_groups([field[i * m : (i + 1) * m] for i in range(n)], length)
            for j in range(n):
                for h in range(copies):
                    packed_ref[h * n + j, f, a] = cells[j]


def finish_kernel(pairs_all, received_ref, passed_ref, out_ref):
    planes, length, lanes = passed_ref.shape
    n = lanes // length
    m = length // n
    copies = received_ref.shape[0] // n
    for a in range(planes):
        cells = []
        for j in range(n):
            total = received_ref[j, a]
            for h in range(1, copies):
                total = total + received_ref[h * n + j, a]
            cells.append(total)
        rows = swap_groups(cells, length)
        for i in range(n):
            out_ref[a, i * m : (i + 1) * m] = passed_ref[a, i * m : (i + 1) * m] + rows[i] * (1.0 / pairs_all)


def fft8(re, im, sign):
    half = 0.7071067811865476

    def four(r, i):
        sr0, si0, dr0, di0 = r[0] + r[2], i[0] + i[2], r[0] - r[2], i[0] - i[2]
        sr1, si1, dr1, di1 = r[1] + r[3], i[1] + i[3], r[1] - r[3], i[1] - i[3]
        if sign > 0:
            tr, ti = -di1, dr1
            return [sr0 + sr1, dr0 - di1, sr0 - sr1, dr0 + di1], [si0 + si1, di0 + dr1, si0 - si1, di0 - dr1]
        return [sr0 + sr1, dr0 + di1, sr0 - sr1, dr0 - di1], [si0 + si1, di0 - dr1, si0 - si1, di0 + dr1]

    ar, ai = [re[j] + re[j + 4] for j in range(4)], [im[j] + im[j + 4] for j in range(4)]
    br, bi = [re[j] - re[j + 4] for j in range(4)], [im[j] - im[j + 4] for j in range(4)]
    if sign > 0:
        br[1], bi[1] = (br[1] - bi[1]) * half, (br[1] + bi[1]) * half
        br[2], bi[2] = -bi[2], br[2]
        br[3], bi[3] = (br[3] + bi[3]) * -half, (br[3] - bi[3]) * half
    else:
        br[1], bi[1] = (br[1] + bi[1]) * half, (bi[1] - br[1]) * half
        br[2], bi[2] = bi[2], -br[2]
        br[3], bi[3] = (bi[3] - br[3]) * half, (br[3] + bi[3]) * -half
    er, ei = four(ar, ai)
    odr, odi = four(br, bi)
    out_re, out_im = [None] * 8, [None] * 8
    for k in range(4):
        out_re[2 * k], out_im[2 * k] = er[k], ei[k]
        out_re[2 * k + 1], out_im[2 * k + 1] = odr[k], odi[k]
    return out_re, out_im


def split(x):
    high = x.astype(BF16)
    return high, (x - high.astype(F32)).astype(BF16)


def dot(a, b):
    return jnp.dot(a, b, preferred_element_type=F32)


def collision_kernel(
    received_ref, g0_ref, g1_ref, g2_ref, g3_ref, lane_real_ref, lane_fwd_ref, lane_inv_ref, row_fwd_ref, row_inv_ref, tw_ref,
    out_ref, cell_ref, v_ref, wide_ref, y_ref, x_ref, z_ref, total_ref, loss_ref,
):
    gains = (g0_ref, g1_ref, g2_ref, g3_ref)
    pairs = len(gains)
    length = row_fwd_ref.shape[0] // 2
    lanes = tw_ref.shape[1]
    m = tw_ref.shape[0] // 2
    rows = m * length
    step = 16
    chunks = [(r, r + step) for r in range(0, length, step)]

    def put_rows(f, at, r, re, im):
        for s, part in enumerate((re, im)):
            high, low = split(part)
            x_ref[f, s * length + r : s * length + r + step, at * lanes : (at + 1) * lanes] = high
            x_ref[f, (2 + s) * length + r : (2 + s) * length + r + step, at * lanes : (at + 1) * lanes] = low

    def twiddles(b1):
        return tw_ref[b1 : b1 + 1, :], tw_ref[m + b1 : m + b1 + 1, :]

    def forward_tail(f):
        for r, e in chunks:
            re, im = [], []
            for b1 in range(m):
                base = (f * m + b1) * length
                yr, yi = y_ref[base + r : base + e, :lanes], y_ref[base + r : base + e, lanes:]
                if b1 > 0:
                    cosine, sine = twiddles(b1)
                    yr, yi = yr * cosine + yi * sine, yi * cosine - yr * sine
                re.append(yr)
                im.append(yi)
            re, im = fft8(re, im, -1)
            for k1 in range(m):
                put_rows(f, k1, r, re[k1], im[k1])
        x = x_ref[f]
        z_ref[f] = dot(row_fwd_ref[...], jnp.concatenate([x, x[: 2 * length]], axis=0))

    def inverse_head(f):
        x = x_ref[f]
        z_ref[f] = dot(row_inv_ref[...], jnp.concatenate([x, x[: 2 * length]], axis=0))
        for r, e in chunks:
            re = [z_ref[f, r:e, k * lanes : (k + 1) * lanes] for k in range(m)]
            im = [z_ref[f, length + r : length + e, k * lanes : (k + 1) * lanes] for k in range(m)]
            re, im = fft8(re, im, 1)
            for b1 in range(m):
                ur, ui = re[b1], im[b1]
                if b1 > 0:
                    cosine, sine = twiddles(b1)
                    ur, ui = ur * cosine - ui * sine, ui * cosine + ur * sine
                base = (f * m + b1) * length
                for s, part in enumerate((ur, ui)):
                    high, low = split(part)
                    wide_ref[base + r : base + e, s * lanes : (s + 1) * lanes] = high
                    wide_ref[base + r : base + e, (2 + s) * lanes : (3 + s) * lanes] = low

    def lane_stage(fields, table):
        wide = wide_ref[: fields * rows]
        return dot(jnp.concatenate([wide, wide[:, : 2 * lanes]], axis=1), table)

    for f in range(2):
        cell_ref[f] = received_ref[:, f].reshape(rows, lanes)
    for b1 in range(m):
        state = cell_ref[0, pl.ds(b1, length, stride=m), :]
        passed = cell_ref[1, pl.ds(b1, length, stride=m), :]
        v_ref[b1 * length : (b1 + 1) * length] = passed
        for f, field in enumerate((state, state * passed)):
            high, low = split(field)
            base = (f * m + b1) * length
            wide_ref[base : base + length, :lanes] = high
            wide_ref[base : base + length, lanes : 2 * lanes] = low
    wide = wide_ref[: 2 * rows, : 2 * lanes]
    y_ref[: 2 * rows] = dot(jnp.concatenate([wide, wide[:, :lanes]], axis=1), lane_real_ref[...])
    forward_tail(0)
    forward_tail(1)

    for k1 in range(m):
        span = slice(k1 * lanes, (k1 + 1) * lanes)
        for r, e in chunks:
            sr, si = z_ref[0, r:e, span], z_ref[0, length + r : length + e, span]
            loss = sum(g[2, r:e, span] for g in gains)
            for p, g in enumerate(gains):
                gl, gr = g[0, r:e, span], g[1, r:e, span]
                put_rows(p, k1, r, gr * sr - gl * si, gr * si + gl * sr)
            put_rows(pairs, k1, r, loss * sr, loss * si)
            qr, qi = z_ref[1, r:e, span], z_ref[1, length + r : length + e, span]
            total_ref[r:e, span] = loss * qi
            total_ref[length + r : length + e, span] = -loss * qr
    for f in range(pairs + 1):
        inverse_head(f)
    y_ref[...] = lane_stage(pairs + 1, lane_inv_ref[...])
    loss_ref[...] = y_ref[pairs * rows :, :lanes] * v_ref[...]

    for p in range(pairs):
        for s in range(2):
            high, low = split(y_ref[p * rows : (p + 1) * rows, s * lanes : (s + 1) * lanes] * v_ref[...])
            wide_ref[p * rows : (p + 1) * rows, s * lanes : (s + 1) * lanes] = high
            wide_ref[p * rows : (p + 1) * rows, (2 + s) * lanes : (3 + s) * lanes] = low
    y_ref[: pairs * rows] = lane_stage(pairs, lane_fwd_ref[...])
    for p in range(pairs):
        forward_tail(p)
    for k1 in range(m):
        span = slice(k1 * lanes, (k1 + 1) * lanes)
        for r, e in chunks:
            tr, ti = total_ref[r:e, span], total_ref[length + r : length + e, span]
            for p, g in enumerate(gains):
                gl, gr = g[0, r:e, span], g[1, r:e, span]
                zr, zi = z_ref[p, r:e, span], z_ref[p, length + r : length + e, span]
                tr = tr + gr * zr - gl * zi
                ti = ti + gr * zi + gl * zr
            put_rows(0, k1, r, tr, ti)
    inverse_head(0)
    y_ref[:rows, :lanes] = lane_stage(1, lane_inv_ref[:, lanes:]) - loss_ref[...]
    for b1 in range(m):
        cell_ref[0, pl.ds(b1, length, stride=m), :] = y_ref[b1 * length : (b1 + 1) * length, :lanes]
    out_ref[...] = cell_ref[0].reshape(out_ref.shape)


def local(adjoint_next, saved_state, gain_left, gain_right):
    planes, length, lanes = adjoint_next.shape
    n = lanes // length
    m = length // n
    tiles, quads = lax.axis_size("tile"), lax.axis_size("quad")
    pairs_all = gain_left.shape[0] * quads
    table_lanes = m * lanes
    quad = lax.axis_index("quad")
    first = (quad * planes).astype(F32).reshape(1)
    ahead = (quad >= quads // 2).astype(jnp.int32).reshape(1)
    towards = [((t + (1 if q >= quads // 2 else -1)) % tiles * quads + q, t * quads + q) for t in range(tiles) for q in range(quads)]
    halo = lax.ppermute(adjoint_next, ("tile", "quad"), towards)

    lane_mirror, row_mirror = make_mirrors(length, n)
    own_gain = pl.pallas_call(
        even_kernel,
        out_shape=jax.ShapeDtypeStruct((3, length, table_lanes), F32),
        in_specs=[VMEM] * 4,
        out_specs=VMEM,
    )(gain_left.reshape(length, table_lanes), gain_right.reshape(length, table_lanes), lane_mirror, row_mirror)
    gains = [own_gain] + [lax.ppermute(own_gain, "quad", [(q, q ^ d) for q in range(quads)]) for d in range(1, n)]

    block = (planes, m, lanes)
    passed, packed = pl.pallas_call(
        pass_kernel,
        out_shape=(
            jax.ShapeDtypeStruct(adjoint_next.shape, F32),
            jax.ShapeDtypeStruct((quads, 2) + block, F32),
        ),
        in_specs=[SMEM, SMEM, VMEM, VMEM, VMEM],
        out_specs=(VMEM, VMEM),
    )(first, ahead, adjoint_next, saved_state, halo)
    received = lax.all_to_all(packed, "quad", 0, 0)

    const = make_constants(length, n)
    rows = m * length
    partial = pl.pallas_call(
        collision_kernel,
        out_shape=jax.ShapeDtypeStruct((quads,) + block, F32),
        in_specs=[VMEM] * (1 + n + 6),
        out_specs=VMEM,
        scratch_shapes=[
            pltpu.VMEM((2, rows, lanes), F32),
            pltpu.VMEM((rows, lanes), F32),
            pltpu.VMEM(((n + 1) * rows, 4 * lanes), BF16),
            pltpu.VMEM(((n + 1) * rows, 2 * lanes), F32),
            pltpu.VMEM((n + 1, 4 * length, table_lanes), BF16),
            pltpu.VMEM((n + 1, 2 * length, table_lanes), F32),
            pltpu.VMEM((2 * length, table_lanes), F32),
            pltpu.VMEM((rows, lanes), F32),
        ],
        compiler_params=pltpu.CompilerParams(vmem_limit_bytes=40 * 1024 * 1024),
    )(
        received, *gains, const["lane_real"], const["lane_fwd"], const["lane_inv"], const["row_fwd"], const["row_inv"], const["twiddle"],
    )
    returned = lax.all_to_all(partial, "quad", 0, 0)
    return pl.pallas_call(
        functools.partial(finish_kernel, pairs_all),
        out_shape=jax.ShapeDtypeStruct(adjoint_next.shape, F32),
        in_specs=[VMEM, VMEM],
        out_specs=VMEM,
    )(returned, passed)


def solution(mesh):
    in_specs = (
        P("quad", None, "tile"),
        P("quad", None, "tile"),
        P("quad", None, None),
        P("quad", None, None),
    )
    out_specs = P("quad", None, "tile")
    return jax.shard_map(local, mesh=mesh, in_specs=in_specs, out_specs=out_specs, check_vma=False)
```

```python
import functools

import jax
import jax.numpy as jnp
import numpy as np
from jax import lax
from jax.experimental import pallas as pl
from jax.experimental.pallas import tpu as pltpu
from jax.sharding import PartitionSpec as P


F32 = jnp.float32
BF16 = jnp.bfloat16
VMEM = pl.BlockSpec(memory_space=pltpu.VMEM)
HBM = pl.BlockSpec(memory_space=pltpu.HBM)
SMEM = pl.BlockSpec(memory_space=pltpu.SMEM)


def split_np(table):
    high = np.asarray(table, np.float32).astype(BF16)
    low = (np.asarray(table, np.float64) - high.astype(np.float64)).astype(BF16)
    return high, low


def make_constants(length, n):
    m = length // n
    lanes = n * length
    b2, c = np.divmod(np.arange(lanes), length)
    turns = np.outer(b2, b2) % n / n + np.outer(c, c) % length / length
    er, ei = np.cos(2 * np.pi * turns), -np.sin(2 * np.pi * turns)
    a = np.arange(length)
    turns = np.outer(a, a) % length / length
    co, si = np.cos(2 * np.pi * turns), np.sin(2 * np.pi * turns)
    high, low = split_np(np.block([[co, si], [-si, co]]))
    theta = 2 * np.pi * np.outer(np.arange(m), b2) / length
    return (
        jnp.asarray(np.stack(split_np(np.block([[er, ei], [-ei, er]])))),
        jnp.asarray(np.concatenate([high, high, low], axis=1)),
        jnp.asarray(np.concatenate([np.cos(theta), np.sin(theta)], axis=0).astype(np.float32)),
    )


def swap_groups(vectors, length):
    v0, v1, v2, v3 = vectors
    lane = lax.broadcasted_iota(jnp.int32, v0.shape, v0.ndim - 1)
    low = lane < 2 * length
    even = lane // length % 2 == 0
    roll = functools.partial(pltpu.roll, axis=v0.ndim - 1)
    a0, a2 = jnp.where(low, v0, roll(v2, 2 * length)), jnp.where(low, roll(v0, 2 * length), v2)
    a1, a3 = jnp.where(low, v1, roll(v3, 2 * length)), jnp.where(low, roll(v1, 2 * length), v3)
    b0, b1 = jnp.where(even, a0, roll(a1, length)), jnp.where(even, roll(a0, 3 * length), a1)
    b2, b3 = jnp.where(even, a2, roll(a3, length)), jnp.where(even, roll(a2, 3 * length), a3)
    return b0, b1, b2, b3


def cells_of(field, length):
    n = field.shape[1] // length
    m = length // n
    return swap_groups([field[i * m : (i + 1) * m] for i in range(n)], length)


def courant(index, length):
    return (index - (length - 1) / 2.0) / length


def local_kernel(first_ref, ahead_ref, adjoint_hbm, state_hbm, base_ref, cells_ref, adjoint_ref, state_ref, sems):
    copies = [
        pltpu.make_async_copy(adjoint_hbm, adjoint_ref, sems.at[0]),
        pltpu.make_async_copy(state_hbm, state_ref, sems.at[1]),
    ]
    for copy in copies:
        copy.start()
    for copy in copies:
        copy.wait()
    planes, length, lanes = adjoint_ref.shape
    lane = lax.broadcasted_iota(jnp.int32, (length, lanes), 1)
    sy = courant(lax.broadcasted_iota(jnp.int32, (length, lanes), 0).astype(F32), length)
    own_lanes = jnp.where(ahead_ref[0] == 1, lane, lanes - 1 - lane) < lanes // 2
    odd = lane // length % 2 == 1
    for a in range(planes):
        centre = adjoint_ref[a]
        one = jnp.where(own_lanes, pltpu.roll(centre, lanes // 2, axis=1), 0.0)
        partner = jnp.where(odd, pltpu.roll(centre, length, axis=1), pltpu.roll(centre, lanes - length, axis=1))
        sx = courant(first_ref[0] + float(a), length)
        base_ref[a] = centre - jnp.abs(sx) * (3.0 * centre - 4.0 * one) / 2.0 - 2.0 * jnp.abs(sy) * (centre - partner)
        for j, cell in enumerate(cells_of(state_ref[a], length)):
            cells_ref[j, a] = cell


def pass_kernel(first_ref, ahead_ref, base_ref, cells_ref, halo_ref, passed_ref, packed_ref):
    planes, length, lanes = base_ref.shape
    n = cells_ref.shape[0]
    lane = lax.broadcasted_iota(jnp.int32, (length, lanes), 1)
    own_lanes = jnp.where(ahead_ref[0] == 1, lane, lanes - 1 - lane) < lanes // 2
    for a in range(planes):
        two = halo_ref[a]
        one = jnp.where(own_lanes, 0.0, pltpu.roll(two, lanes // 2, axis=1))
        sx = courant(first_ref[0] + float(a), length)
        passed = base_ref[a] - jnp.abs(sx) * (two - 4.0 * one) / 2.0
        passed_ref[a] = passed
        for j, cell in enumerate(cells_of(passed, length)):
            for q in range(j, packed_ref.shape[0], n):
                packed_ref[q, 0, a] = cells_ref[j, a]
                packed_ref[q, 1, a] = cell


def finish_kernel(pairs_all, received_ref, passed_ref, out_ref):
    planes, length, lanes = passed_ref.shape
    n = lanes // length
    m = length // n
    copies = received_ref.shape[0] // n
    for a in range(planes):
        cells = []
        for j in range(n):
            total = received_ref[j, a]
            for h in range(1, copies):
                total = total + received_ref[h * n + j, a]
            cells.append(total)
        rows = swap_groups(cells, length)
        for i in range(n):
            out_ref[a, i * m : (i + 1) * m] = passed_ref[a, i * m : (i + 1) * m] + rows[i] * (1.0 / pairs_all)


def fft8(re, im):
    half = 0.7071067811865476

    def four(r, i):
        sr0, si0, dr0, di0 = r[0] + r[2], i[0] + i[2], r[0] - r[2], i[0] - i[2]
        sr1, si1, dr1, di1 = r[1] + r[3], i[1] + i[3], r[1] - r[3], i[1] - i[3]
        return [sr0 + sr1, dr0 + di1, sr0 - sr1, dr0 - di1], [si0 + si1, di0 - dr1, si0 - si1, di0 + dr1]

    ar, ai = [re[j] + re[j + 4] for j in range(4)], [im[j] + im[j + 4] for j in range(4)]
    br, bi = [re[j] - re[j + 4] for j in range(4)], [im[j] - im[j + 4] for j in range(4)]
    br[1], bi[1] = (br[1] + bi[1]) * half, (bi[1] - br[1]) * half
    br[2], bi[2] = bi[2], -br[2]
    br[3], bi[3] = (bi[3] - br[3]) * half, (br[3] + bi[3]) * -half
    even_re, even_im = four(ar, ai)
    odd_re, odd_im = four(br, bi)
    return [v for pair in zip(even_re, odd_re) for v in pair], [v for pair in zip(even_im, odd_im) for v in pair]


def split(x):
    high = x.astype(BF16)
    return high, (x - high.astype(F32)).astype(BF16)


def dot(a, b):
    return jnp.dot(a, b, preferred_element_type=F32)


class Stages:
    def __init__(self, lane_ref, row_ref, tw_ref, wide_ref, y_ref, x_ref, z_ref):
        self.lane, self.row, self.tw = lane_ref, row_ref, tw_ref
        self.wide, self.y, self.x, self.z = wide_ref, y_ref, x_ref, z_ref
        self.lanes = tw_ref.shape[1]
        self.m = tw_ref.shape[0] // 2
        self.length = z_ref.shape[1] // 2
        self.rows = self.m * self.length
        self.step = 16
        self.chunks = [(r, r + self.step) for r in range(0, self.length, self.step)]

    def span(self, k):
        return slice(k * self.lanes, (k + 1) * self.lanes)

    def put_rows(self, f, at, r, re, im):
        for s, part in enumerate((re, im)):
            high, low = split(part)
            self.x[f, s * self.length + r : s * self.length + r + self.step, self.span(at)] = high
            self.x[f, (2 + s) * self.length + r : (2 + s) * self.length + r + self.step, self.span(at)] = low

    def put_wide(self, base, count, s, part, parts):
        high, low = split(part)
        self.wide[base : base + count, self.span(s)] = high
        self.wide[base : base + count, self.span(parts + s)] = low

    def twiddles(self, b1):
        return self.tw[b1 : b1 + 1, :], self.tw[self.m + b1 : self.m + b1 + 1, :]

    def row_stage(self, f):
        x = self.x[f]
        self.z[f] = dot(self.row[...], jnp.concatenate([x, x[: 2 * self.length]], axis=0))

    def lane_stage(self, fields, parts, at=0):
        wide = self.wide[: fields * self.rows, : 2 * parts * self.lanes]
        high, low = self.lane[0, : parts * self.lanes, at:], self.lane[1, : parts * self.lanes, at:]
        wide = jnp.concatenate([wide, wide[:, : parts * self.lanes]], axis=1)
        return dot(wide, jnp.concatenate([high, high, low], axis=0))

    def forward_tail(self, f):
        for r, e in self.chunks:
            re, im = [], []
            for b1 in range(self.m):
                base = (f * self.m + b1) * self.length
                yr, yi = self.y[base + r : base + e, : self.lanes], self.y[base + r : base + e, self.lanes :]
                if b1 > 0:
                    cosine, sine = self.twiddles(b1)
                    yr, yi = yr * cosine + yi * sine, yi * cosine - yr * sine
                re.append(yr)
                im.append(yi)
            re, im = fft8(re, im)
            for k1 in range(self.m):
                self.put_rows(f, k1, r, re[k1], im[k1])
        self.row_stage(f)

    def inverse_head(self, f):
        self.row_stage(f)
        for r, e in self.chunks:
            re = [self.z[f, r:e, self.span(k)] for k in range(self.m)]
            im = [self.z[f, self.length + r : self.length + e, self.span(k)] for k in range(self.m)]
            re, im = fft8(re, im)
            for b1 in range(self.m):
                ur, ui = re[b1], im[b1]
                if b1 > 0:
                    cosine, sine = self.twiddles(b1)
                    ur, ui = ur * cosine + ui * sine, ui * cosine - ur * sine
                base = (f * self.m + b1) * self.length
                self.put_wide(base + r, self.step, 0, ur, 2)
                self.put_wide(base + r, self.step, 1, ui, 2)


def even_tables(tables, store, length, lanes, m):
    n = lanes // length
    rows = 8
    count = length // rows
    sub = lax.broadcasted_iota(jnp.int32, (rows, lanes), 0)
    lane = lax.broadcasted_iota(jnp.int32, (rows, lanes), 1)
    sub_source = (rows - sub) % rows
    lane_source = (n - lane // length) % n * length + (length - lane % length) % length
    for i, table in enumerate(tables):
        for r in range(count):
            near, far = -r % count, (-r - 1) % count
            mixed = [jnp.where(sub == 0, table(near, g), table(far, g)) for g in range(m)]
            for g in range(m):
                source = jnp.where(lane < length, mixed[-g % m], mixed[(-g - 1) % m])
                source = jnp.take_along_axis(source, sub_source, axis=0, mode="promise_in_bounds")
                source = jnp.take_along_axis(source, lane_source, axis=1, mode="promise_in_bounds")
                store(i, r, g, table(r, g) + source)


def even_kernel(*refs):
    gain_refs, g_ref, product_ref = refs[:-2], refs[-2], refs[-1]
    length = product_ref.shape[0]
    lanes = 128
    m = product_ref.shape[1] // lanes
    scale = 0.5 / length**3

    def tile(ref):
        return lambda r, g: ref[r * 8 : r * 8 + 8, g * lanes : (g + 1) * lanes]

    def store(i, r, g, value):
        g_ref[i, r * 8 : r * 8 + 8, g * lanes : (g + 1) * lanes] = value * scale

    product_ref[...] = sum(left[...] * right[...] for left, right in zip(gain_refs[::2], gain_refs[1::2]))
    even_tables([tile(ref) for ref in gain_refs] + [tile(product_ref)], store, length, lanes, m)


def collision_kernel(
    pairs, received_ref, g_ref, lane_ref, row_ref, tw_ref, out_ref, cell_ref, state_cell_ref, v_ref, loss_ref, total_ref,
    wide_ref, y_ref, x_ref, z_ref,
):
    st = Stages(lane_ref, row_ref, tw_ref, wide_ref, y_ref, x_ref, z_ref)
    length, lanes, m, rows = st.length, st.lanes, st.m, st.rows
    state_cell_ref[...] = received_ref[:, 0].reshape(rows, lanes)
    cell_ref[...] = received_ref[:, 1].reshape(rows, lanes)
    for b1 in range(m):
        state = state_cell_ref[pl.ds(b1, length, stride=m), :]
        passed = cell_ref[pl.ds(b1, length, stride=m), :]
        v_ref[b1 * length : (b1 + 1) * length] = passed
        st.put_wide(b1 * length, length, 0, state, 1)
        st.put_wide(rows + b1 * length, length, 0, state * passed, 1)
    y_ref[: 2 * rows] = st.lane_stage(2, 1)
    st.forward_tail(0)
    st.forward_tail(1)

    for k1 in range(m):
        for r, e in st.chunks:
            span = st.span(k1)
            sr, si = z_ref[0, r:e, span], z_ref[0, length + r : length + e, span]
            for p in range(pairs):
                gl, gr = g_ref[2 * p, r:e, span], g_ref[2 * p + 1, r:e, span]
                st.put_rows(p, k1, r, gr * sr - gl * si, -(gr * si + gl * sr))
            loss = g_ref[2 * pairs, r:e, span]
            st.put_rows(pairs, k1, r, loss * sr, -loss * si)
            total_ref[r:e, span] = loss * z_ref[1, length + r : length + e, span]
            total_ref[length + r : length + e, span] = -loss * z_ref[1, r:e, span]
    for f in range(pairs + 1):
        st.inverse_head(f)
    y_ref[...] = st.lane_stage(pairs + 1, 2)
    loss_ref[...] = y_ref[pairs * rows :, :lanes] * v_ref[...]

    for p in range(pairs):
        for s in range(2):
            part = y_ref[p * rows : (p + 1) * rows, st.span(s)] * v_ref[...]
            st.put_wide(p * rows, rows, s, part if s == 0 else -part, 2)
    y_ref[: pairs * rows] = st.lane_stage(pairs, 2)
    for p in range(pairs):
        st.forward_tail(p)
    for k1 in range(m):
        for r, e in st.chunks:
            span = st.span(k1)
            tr, ti = total_ref[r:e, span], total_ref[length + r : length + e, span]
            for p in range(pairs):
                gl, gr = g_ref[2 * p, r:e, span], g_ref[2 * p + 1, r:e, span]
                zr, zi = z_ref[p, r:e, span], z_ref[p, length + r : length + e, span]
                tr = tr + gr * zr - gl * zi
                ti = ti + gr * zi + gl * zr
            st.put_rows(0, k1, r, tr, -ti)
    st.inverse_head(0)
    y_ref[:rows, :lanes] = st.lane_stage(1, 2, lanes) + loss_ref[...]
    for b1 in range(m):
        cell_ref[pl.ds(b1, length, stride=m), :] = -y_ref[b1 * length : (b1 + 1) * length, :lanes]
    out_ref[...] = cell_ref[...].reshape(out_ref.shape)


def call(kernel, out_shape, in_specs, scratch=(), vmem=4, us=1):
    out_specs = jax.tree.map(lambda _: VMEM, out_shape)
    return pl.pallas_call(
        kernel,
        out_shape=out_shape,
        in_specs=in_specs,
        out_specs=out_specs,
        scratch_shapes=list(scratch),
        cost_estimate=pl.CostEstimate(flops=us * 100_000_000, bytes_accessed=1 << 20, transcendentals=0),
        compiler_params=pltpu.CompilerParams(vmem_limit_bytes=vmem * 1024 * 1024),
    )


def local(adjoint_next, saved_state, gain_left, gain_right):
    planes, length, lanes = adjoint_next.shape
    n = lanes // length
    m = length // n
    rows = m * length
    tiles, quads = lax.axis_size("tile"), lax.axis_size("quad")
    pairs_all = gain_left.shape[0] * quads
    table = (length, m * lanes)
    block = (planes, m, lanes)
    quad = lax.axis_index("quad")
    shaped = jax.ShapeDtypeStruct
    first = (quad * planes).astype(F32).reshape(1)
    ahead = (quad >= quads // 2).astype(jnp.int32).reshape(1)
    towards = [((t + (1 if q >= quads // 2 else -1)) % tiles * quads + q, t * quads + q) for t in range(tiles) for q in range(quads)]
    halo = lax.ppermute(adjoint_next, ("tile", "quad"), towards)

    left, right = gain_left.reshape(table), gain_right.reshape(table)
    carried = jnp.where(lax.axis_index("tile") % 2 == 0, left, right)
    gains = [left, right]
    for d in range(1, n):
        other = lax.ppermute(carried, "quad", [(q, q ^ d) for q in range(quads)])
        gains += [other, lax.ppermute(other, "tile", [(t, t ^ 1) for t in range(tiles)])]

    by_plane, by_cell = shaped((planes, length, lanes), F32), shaped((n,) + block, F32)
    base, cells = call(
        local_kernel,
        (by_plane, by_cell),
        [SMEM, SMEM, HBM, HBM],
        [pltpu.VMEM((planes, length, lanes), F32), pltpu.VMEM((planes, length, lanes), F32), pltpu.SemaphoreType.DMA((2,))],
    )(first, ahead, adjoint_next, saved_state)
    passed, packed = call(pass_kernel, (by_plane, shaped((quads, 2) + block, F32)), [SMEM, SMEM] + [VMEM] * 3)(
        first, ahead, base, cells, halo
    )
    received = lax.all_to_all(packed, "quad", 0, 0)

    g = call(even_kernel, shaped((2 * n + 1,) + table, F32), [VMEM] * (2 * n), [pltpu.VMEM(table, F32)])(*gains)
    cell = pltpu.VMEM((rows, lanes), F32)
    partial = call(
        functools.partial(collision_kernel, n),
        shaped((quads,) + block, F32),
        [VMEM] * 5,
        [
            cell,
            cell,
            cell,
            cell,
            pltpu.VMEM((2 * length, m * lanes), F32),
            pltpu.VMEM(((n + 1) * rows, 4 * lanes), BF16),
            pltpu.VMEM(((n + 1) * rows, 2 * lanes), F32),
            pltpu.VMEM((n + 1, 4 * length, m * lanes), BF16),
            pltpu.VMEM((n + 1, 2 * length, m * lanes), F32),
        ],
        vmem=20,
        us=4,
    )(received, g, *make_constants(length, n))
    returned = lax.all_to_all(partial, "quad", 0, 0)
    return call(functools.partial(finish_kernel, pairs_all), shaped(adjoint_next.shape, F32), [VMEM, VMEM])(returned, passed)


def solution(mesh):
    in_specs = (
        P("quad", None, "tile"),
        P("quad", None, "tile"),
        P("quad", None, None),
        P("quad", None, None),
    )
    out_specs = P("quad", None, "tile")
    return jax.shard_map(local, mesh=mesh, in_specs=in_specs, out_specs=out_specs, check_vma=False)
```
